128 devices in a mesh: aa: 16 (over x, z), ba: 8 (over y, core).
Axes of the slice: x: 4, y: 4, z: 4, core: 2. Of those that a mesh axis runs over, the one named last changes fastest.
Arguments:
- grid_features: bfloat16 [128, 128, 256, 128], P('aa', 'ba'), may hold values from -6 to 6
- weight_real: bfloat16 [32, 32, 16, 128, 128], P('ba', None, 'aa'), may hold values from -6 to 6
- weight_imag: bfloat16 [32, 32, 16, 128, 128], P('ba', None, 'aa'), may hold values from -6 to 6
- mode_keep: int32 [32, 16], P('ba', 'aa'), may hold values from 1 to 16, as said below
- local_weight: bfloat16 [128, 128], replicated, may hold values from -0.5 to 0.5
- local_bias: bfloat16 [128], replicated, may hold values from -3 to 3
Outputs:
- layer_output: bfloat16 [128, 128, 256, 128], P('aa', 'ba')
The draws below stay inside these ranges and needn't reach their ends.
Inputs may be any that keep to these rules, and one draw needn't show every extreme that they name: mode_keep[i, k] counts the retained levels of the second frequency on the line of the i-th retained first frequency and the k-th third frequency.
All inputs are finite; a program needn't handle non-finite values.
Results may differ from the reference program's by a relative error of at most 0.012.
Values may be sent and summed in bfloat16 or wider, within the bound.
A program may use at most 128 MiB of HBM per device.

```python
import math
import jax
import jax.numpy as jnp
from jax import lax

NX = 128
NY = 128
NZ = 256
C = 128
KX = 32
KY = 32
KZ = 16
N_AA = 16


def draw_mode_keep(key, part):
    top_level = KY // 2
    positions = jnp.arange(KX, dtype=jnp.int32)
    level_first = jnp.where(positions < KX // 2, positions, KX - 1 - positions)
    level_third = jnp.arange(KZ, dtype=jnp.int32)
    reach_total = KX // 2 + KZ
    base_level = top_level - (level_first[:, None] + level_third[None, :]) * top_level // reach_total
    jitter = jax.random.randint(key, (KX, KZ), -3, 4, dtype=jnp.int32)
    kept_levels = jnp.clip(base_level + jitter, 1, top_level)
    kept_levels = kept_levels.at[0, 0].set(top_level)
    kept_levels = kept_levels.at[KX // 2 - 1, KZ - 1].set(1)
    return kept_levels.astype(jnp.int32)


def block_levels(own_key, dims, shards, low, top_value):
    def one(dim, shards_of):
        draws = jax.random.uniform(jax.random.fold_in(jax.random.fold_in(own_key, 6), dim), (shards_of,), jnp.float32, low / len(shards), top_value / len(shards))
        return jnp.repeat(jnp.exp(draws), dims[dim] // shards_of).reshape((-1,) + (1,) * (len(dims) - dim - 1))

    gain = one(*shards[0])
    for cut in shards[1:]:
        gain = gain * one(*cut)
    return gain


def centred(rng, extent, spread, limit, pieces=(), kind=jnp.bfloat16):
    drawn = jax.random.normal(rng, extent, jnp.float32) * spread
    if len(pieces) > 0:
        drawn = block_levels(rng, extent, pieces, -0.22, 0.18) * drawn
    return jnp.clip(drawn, min=-limit, max=limit).astype(kind)


def setup_inputs(seed: int = 0) -> dict:
    keys = jax.random.split(jax.random.key(seed), 7)
    grid_features = centred(keys[0], (NX, NY, NZ, C), 1.0, 6.0, ((0, 16), (1, 8)))
    weight_real = centred(keys[1], (KX, KY, KZ, C, C), 1.0, 6.0, ((0, 8), (2, 16)))
    weight_imag = centred(keys[2], (KX, KY, KZ, C, C), 1.0, 6.0, ((0, 8), (2, 16)))
    mode_keep = draw_mode_keep(jax.random.fold_in(keys[6], 71), 0)
    local_weight = centred(keys[4], (C, C), C ** -0.5, 0.5)
    local_bias = centred(keys[5], (C,), 0.5, 3.0)
    return {"grid_features": grid_features, "weight_real": weight_real, "weight_imag": weight_imag, "mode_keep": mode_keep, "local_weight": local_weight, "local_bias": local_bias}


highest = lax.Precision.HIGHEST


def kept_modes(length, number):
    positions = jnp.arange(number, dtype=jnp.int32)
    return jnp.where(positions < number // 2, positions, positions + (length - number)).astype(jnp.int32)


def phase_tables(length, mode_list):
    places = jnp.arange(length, dtype=jnp.int32)
    phase_steps = (places[:, None] * mode_list[None, :]) % length
    angles = phase_steps.astype(jnp.float32) * (2.0 * math.pi / length)
    return jnp.cos(angles), jnp.sin(angles)


def forward_kernel(length, number):
    cosine_table, sine_table = phase_tables(length, kept_modes(length, number))
    upper_rows = jnp.concatenate([cosine_table, -sine_table], axis=1)
    lower_rows = jnp.concatenate([sine_table, cosine_table], axis=1)
    return jnp.concatenate([upper_rows, lower_rows], axis=0)


def inverse_kernel(length, number):
    cosine_table, sine_table = phase_tables(length, kept_modes(length, number))
    upper_rows = jnp.concatenate([cosine_table.T, sine_table.T], axis=1)
    lower_rows = jnp.concatenate([-sine_table.T, cosine_table.T], axis=1)
    return jnp.concatenate([upper_rows, lower_rows], axis=0)


def depth_kernels():
    cosine_table, sine_table = phase_tables(NZ, jnp.arange(KZ, dtype=jnp.int32))
    forward = jnp.concatenate([cosine_table, -sine_table], axis=1).astype(jnp.bfloat16)
    factor = jnp.where(jnp.arange(KZ, dtype=jnp.int32) == 0, 1.0, 2.0).astype(jnp.float32) / (NX * NY * NZ)
    inverse = jnp.concatenate([cosine_table.T * factor[:, None], -sine_table.T * factor[:, None]], axis=0).astype(jnp.bfloat16)
    return forward, inverse


def along_first(operand, kernel):
    return jnp.einsum('pabc,pq->qabc', operand, kernel, precision=highest, preferred_element_type=jnp.float32)


def along_second(operand, kernel):
    return jnp.einsum('apbc,pq->aqbc', operand, kernel, precision=highest, preferred_element_type=jnp.float32)


def mode_mask(kept_counts):
    positions = jnp.arange(KY, dtype=jnp.int32)
    levels = jnp.where(positions < KY // 2, positions, KY - 1 - positions)
    return (levels[None, :, None] < kept_counts[:, None, :]).astype(jnp.float32)


def reference(grid_features, weight_real, weight_imag, mode_keep, local_weight, local_bias):
    forward_depth, inverse_depth = depth_kernels()
    slab_rows = NX // N_AA
    field_slabs = grid_features.reshape(N_AA, slab_rows, NY, NZ, C)

    def depth_forward(slab_cells):
        flat_rows = jnp.transpose(slab_cells, (0, 1, 3, 2)).reshape(slab_rows * NY * C, NZ).astype(jnp.float32)
        coeffs = jnp.dot(flat_rows, forward_depth.astype(jnp.float32), precision=highest, preferred_element_type=jnp.float32)
        coeffs = jnp.transpose(coeffs.reshape(slab_rows, NY, C, 2 * KZ), (0, 1, 3, 2))
        return coeffs.astype(jnp.bfloat16)

    coeffs = lax.map(depth_forward, field_slabs).reshape(NX, NY, 2 * KZ, C)
    stacked = jnp.concatenate([coeffs[:, :, :KZ], coeffs[:, :, KZ:]], axis=0).astype(jnp.float32)
    result = along_first(stacked, forward_kernel(NX, KX))
    result = jnp.concatenate([result[:KX], result[KX:]], axis=1)
    result = along_second(result, forward_kernel(NY, KY)).astype(jnp.bfloat16)
    spec_real = result[:, :KY]
    spec_imag = result[:, KY:]

    def mix_line(operands):
        real_part, imag_part, line_real, line_imag = operands
        real_part = real_part.astype(jnp.float32)
        imag_part = imag_part.astype(jnp.float32)
        line_real = line_real.astype(jnp.float32)
        line_imag = line_imag.astype(jnp.float32)
        pattern = 'bcd,bcde->bce'
        out_real = jnp.einsum(pattern, real_part, line_real, precision=highest) - jnp.einsum(pattern, imag_part, line_imag, precision=highest)
        out_imag = jnp.einsum(pattern, real_part, line_imag, precision=highest) + jnp.einsum(pattern, imag_part, line_real, precision=highest)
        return out_real, out_imag

    mixed_real, mixed_imag = lax.map(mix_line, (spec_real, spec_imag, weight_real, weight_imag))
    keep_mask = mode_mask(mode_keep)[..., None]
    mixed_real = mixed_real * keep_mask
    mixed_imag = mixed_imag * keep_mask
    result = along_second(jnp.concatenate([mixed_real, mixed_imag], axis=1), inverse_kernel(NY, KY))
    result = jnp.concatenate([result[:, :NY], result[:, NY:]], axis=0)
    result = along_first(result, inverse_kernel(NX, KX)).astype(jnp.bfloat16)
    back_field = jnp.concatenate([result[:NX], result[NX:]], axis=2)
    back_slabs = back_field.reshape(N_AA, slab_rows, NY, 2 * KZ, C)

    def finish_slab(operands):
        slab_cells, back_slab = operands
        flat_rows = jnp.transpose(back_slab, (0, 1, 3, 2)).reshape(slab_rows * NY * C, 2 * KZ).astype(jnp.float32)
        spectral = jnp.dot(flat_rows, inverse_depth.astype(jnp.float32), precision=highest, preferred_element_type=jnp.float32)
        spectral = jnp.transpose(spectral.reshape(slab_rows, NY, C, NZ), (0, 1, 3, 2))
        local_term = jnp.dot(slab_cells.reshape(-1, C).astype(jnp.float32), local_weight.astype(jnp.float32), precision=highest, preferred_element_type=jnp.float32)
        local_term = local_term.reshape(slab_rows, NY, NZ, C)
        return jax.nn.gelu(spectral + local_term + local_bias.astype(jnp.float32)).astype(jnp.bfloat16)

    return lax.map(finish_slab, (field_slabs, back_slabs)).reshape(NX, NY, NZ, C)
```

```python
import numpy as np
import jax
import jax.numpy as jnp
from jax import lax
from jax.experimental import pallas as pl
from jax.experimental.pallas import tpu as pltpu
from jax.sharding import PartitionSpec as P

NX, NY, NZ, C = 128, 128, 256, 128
KX, KY, KZ = 32, 32, 16
NA, NB = 16, 8
MESH = pl.DeviceIdType.MESH
BF = jnp.bfloat16
F32 = jnp.float32

AA_ORDER = [(1, 0), (0, 1), (3, 0), (0, 3), (2, 0), (0, 2), (1, 1), (3, 3), (1, 3), (3, 1),
            (2, 1), (2, 3), (1, 2), (3, 2), (2, 2)]
BA_ORDER = [(1, 0), (3, 0), (2, 0), (1, 1), (3, 1), (2, 1), (0, 1)]


def kept(length, number):
    j = np.arange(number)
    return np.where(j < number // 2, j, j + length - number)


def angle(k, n, length):
    return 2.0 * np.pi * ((k * n) % length) / length


def complex_block(theta, ri_out, ri_in, sign):
    c, s = np.cos(theta), sign * np.sin(theta)
    return np.where(ri_out == ri_in, c, np.where(ri_out == 0, -s, s))


def tables():
    kx, ky = kept(NX, KX), kept(NY, KY)
    k, _, r, z = np.ix_(np.arange(KZ), np.arange(4), np.arange(2), np.arange(NZ))
    th = angle(k, z, NZ)
    t1 = np.where(r == 0, np.cos(th), -np.sin(th)) + np.zeros((KZ, 4, 2, NZ))
    t1 = t1.reshape(128, 256)
    k, _, r, x, q = np.ix_(kx, np.arange(4), np.arange(2), np.arange(NX), np.arange(2))
    t2 = complex_block(angle(k, x, NX), r, q, -1) + np.zeros((KX, 4, 2, NX, 2))
    t2 = t2.reshape(256, 256)
    k, r, h, b, y, q = np.ix_(ky, np.arange(2), np.arange(2), np.arange(NB), np.arange(8), np.arange(2))
    f = complex_block(angle(k, b * 16 + h * 8 + y, NY), r, q, -1).reshape(KY, 2, 256)
    t3 = np.concatenate([f.reshape(64, 256), np.stack([-f[:, 1], f[:, 0]], axis=1).reshape(64, 256)], axis=0)
    h, b, y, m, r, n, k, q = np.ix_(np.arange(2), np.arange(NB), np.arange(8), np.arange(4), np.arange(2),
                                    np.arange(4), ky, np.arange(2))
    t4 = complex_block(angle(k, b * 16 + h * 8 + y, NY), r, q, 1) * (m == n)
    t4 = t4.reshape(1024, 256)
    y, x, r, b, w, m, q = np.ix_(np.arange(2), np.arange(NX), np.arange(2), np.arange(NB), np.arange(2),
                                 np.arange(4), np.arange(2))
    t5 = complex_block(angle(kx[b * 4 + m], x, NX), r, q, 1) * (y == w)
    t5 = t5.reshape(512, 128)
    z, k, _, r = np.ix_(np.arange(NZ), np.arange(KZ), np.arange(8), np.arange(2))
    th = angle(k, z, NZ)
    t6 = np.where(r == 0, np.cos(th), -np.sin(th)) * np.where(k == 0, 1.0, 2.0) / (NX * NY * NZ) * 0.5
    t6 = (t6 + np.zeros((NZ, KZ, 8, 2))).reshape(256, 256)
    return [np.asarray(t, np.float32).astype(jnp.bfloat16) for t in (t1, t2, t3, t4, t5, t6)]


def dot(a, b):
    return jnp.dot(a, b, preferred_element_type=F32)


def spectral_kernel(x_hbm, wr_hbm, wi_hbm, keep_ref, t1_hbm, t2_hbm, t3_hbm, t4_hbm, t5_hbm, out_ref,
                    xv, wv, t1v, t1m, t2v, t2m, t3v, t4v, t5v, s1, r1, s2, r2, s3, r3, s4,
                    xsem, wsem, tsem, sa, ra, sb, rb, sc, rc, sd, rd):
    ia, ib = lax.axis_index("aa"), lax.axis_index("ba")
    ix, iz, iy, ic = ia // 4, lax.rem(ia, 4), ib // 2, lax.rem(ib, 2)
    aa_peers = [lax.rem(ix + dx, 4) * 4 + lax.rem(iz + dz, 4) for dx, dz in AA_ORDER]
    ba_peers = [lax.rem(iy + dy, 4) * 2 + lax.rem(ic + dc, 2) for dy, dc in BA_ORDER]

    tcopies = [pltpu.make_async_copy(src, dst, tsem.at[i]) for i, (src, dst) in enumerate(
        [(t1_hbm, t1v), (t2_hbm, t2v), (t3_hbm, t3v), (t4_hbm, t4v), (t5_hbm, t5v)])]
    tcopies[0].start()
    xcopies = [pltpu.make_async_copy(x_hbm.at[:, pl.ds(4 * g, 4)], xv.at[g], xsem.at[g]) for g in range(4)]
    for c in xcopies:
        c.start()
    tcopies[1].start()
    wcopies = [pltpu.make_async_copy(wr_hbm, wv.at[0], wsem.at[0]), pltpu.make_async_copy(wi_hbm, wv.at[1], wsem.at[1])]

    barrier = pltpu.get_barrier_semaphore()
    for t in aa_peers:
        pl.semaphore_signal(barrier, inc=1, device_id={"aa": t}, device_id_type=MESH)
    for t in ba_peers:
        pl.semaphore_signal(barrier, inc=1, device_id={"ba": t}, device_id_type=MESH)

    def send_aa(src, dst, ssem, rsem):
        for t in aa_peers:
            pltpu.make_async_remote_copy(src.at[t], dst.at[ia], ssem, rsem, device_id={"aa": t}, device_id_type=MESH).start()

    def send_ba(src, dst, ssem, rsem):
        for t in ba_peers:
            pltpu.make_async_remote_copy(src(t), dst.at[ib], ssem, rsem, device_id={"ba": t}, device_id_type=MESH).start()

    def wait_bytes(ref, sem):
        pltpu.make_async_copy(ref, ref, sem).wait()

    tcopies[0].wait()
    rows1 = lax.broadcasted_iota(jnp.int32, (128, 256), 0) // 2 % 4
    for i in range(4):
        t1m[i] = jnp.where(rows1 == i, t1v[...].astype(F32), 0.0).astype(BF)
    for g in range(4):
        xcopies[g].wait()
        for y in range(4):
            acc = None
            for i in range(4):
                rhs = jnp.concatenate([xv[g, i, y], xv[g, i + 4, y]], axis=1)
                p = dot(t1m[i], rhs)
                acc = p if acc is None else acc + p
            acc = acc.reshape(KZ, 8, 256)
            s1[g, :, y] = jnp.concatenate([acc[:, :, :128], acc[:, :, 128:]], axis=1).astype(BF)
        if g == 0:
            pl.semaphore_wait(barrier, len(aa_peers) + len(ba_peers))
        send_aa(s1.at[g], r1.at[g], sa, ra.at[g])
        r1[g, ia] = s1[g, ia]

    for c in tcopies[2:] + wcopies:
        c.start()
    tcopies[1].wait()
    rows2 = lax.broadcasted_iota(jnp.int32, (256, 256), 0) // 2 % 4
    for i in range(4):
        t2m[i] = jnp.where(rows2 == i, t2v[...].astype(F32), 0.0).astype(BF)

    for h in range(2):
        for g in (2 * h, 2 * h + 1):
            wait_bytes(r1.at[g, pl.ds(0, NA - 1)], ra.at[g])
        acc = None
        for i in range(4):
            rhs = jnp.concatenate([r1[2 * h, :, i].reshape(256, C), r1[2 * h + 1, :, i].reshape(256, C)], axis=1)
            p = dot(t2m[i], rhs)
            acc = p if acc is None else acc + p
        acc = acc.reshape(KX, 8, 256)
        s2[h] = jnp.concatenate([acc[:, :, :128], acc[:, :, 128:]], axis=1).astype(BF)
        send_ba(lambda t: s2.at[h, pl.ds(4 * t, 4)], r2.at[h], sb, rb.at[h])
        r2[h, ib] = s2[h, pl.ds(4 * ib, 4)]

    for c in tcopies[2:]:
        c.wait()
    for c in wcopies:
        c.wait()
    for h in range(2):
        wait_bytes(r2.at[h, pl.ds(0, NB - 1)], rb.at[h])

    row16 = lax.broadcasted_iota(jnp.int32, (16, 256), 0) // 2 % 4
    row8 = lax.broadcasted_iota(jnp.int32, (8, C), 0) // 2
    mixed = [[], [], [], []]
    for p in range(2):
        rhs = jnp.concatenate([r2[:, :, 2 * p].reshape(256, C), r2[:, :, 2 * p + 1].reshape(256, C)], axis=1)
        spec = dot(t3v[...], rhs)
        for q in range(8):
            first, second = spec[8 * q:8 * q + 8], spec[64 + 8 * q:64 + 8 * q + 8]
            lhs = jnp.concatenate([jnp.concatenate([first[:, :C], first[:, C:]], axis=0),
                                   jnp.concatenate([second[:, :C], second[:, C:]], axis=0)], axis=1)
            acc = None
            for j in range(4):
                k = 4 * q + j
                w = jnp.concatenate([jnp.concatenate([wv[r, 2 * p, k], wv[r, 2 * p + 1, k]], axis=1) for r in range(2)], axis=0)
                part = dot(jnp.where(row16 == j, lhs, 0.0).astype(BF), w)
                acc = part if acc is None else acc + part
            position = 4 * q + row8
            level = jnp.where(position < KY // 2, position, KY - 1 - position)
            mixed[2 * p].append(jnp.where(level < keep_ref[2 * p, 0], acc[:8, :C], 0.0))
            mixed[2 * p + 1].append(jnp.where(level < keep_ref[2 * p + 1, 0], acc[8:, C:], 0.0))
    rhs = jnp.concatenate([m for line in mixed for m in line], axis=0).astype(BF)
    for h in range(2):
        s3[h] = dot(t4v[pl.ds(512 * h, 512)], rhs).astype(BF).reshape(NB, 4, 16, C)
        send_ba(lambda t: s3.at[h, t], r3.at[h], sc, rc.at[h])
        r3[h, ib] = s3[h, ib]

    for h in range(2):
        wait_bytes(r3.at[h, pl.ds(0, NB - 1)], rc.at[h])
        for g in (2 * h, 2 * h + 1):
            n = 2 * (g - 2 * h)
            rhs = jnp.concatenate([r3[h, :, n].reshape(128, C), r3[h, :, n + 1].reshape(128, C)], axis=1)
            back = dot(t5v[...], rhs).astype(BF)
            for half in range(2):
                for i in range(2):
                    s4[g, :, 2 * half + i] = back[256 * i:256 * i + 256, C * half:C * half + C].reshape(NA, 16, C)
            send_aa(s4.at[g], out_ref.at[g], sd, rd.at[g])
            out_ref[g, ia] = s4[g, ia]

    for g in range(4):
        wait_bytes(out_ref.at[g, pl.ds(0, NA - 1)], rd.at[g])
    wait_bytes(s1.at[:, pl.ds(0, NA - 1)], sa)
    wait_bytes(s4.at[:, pl.ds(0, NA - 1)], sd)
    wait_bytes(r2.at[:, pl.ds(0, NB - 1)], sb)
    wait_bytes(r3.at[:, pl.ds(0, NB - 1)], sc)


def final_kernel(x_ref, back_ref, w_ref, bias_ref, t6_ref, out_ref, t6m, wbd):
    j, xh = pl.program_id(0), pl.program_id(1)

    @pl.when((j == 0) & (xh == 0))
    def _():
        lane = lax.broadcasted_iota(jnp.int32, (256, 256), 1) // 2 % 8
        for i in range(8):
            t6m[i] = jnp.where(lane == i, t6_ref[...].astype(F32), 0.0).astype(BF)
        w = (w_ref[...].astype(F32) * 0.5).astype(BF)
        z = jnp.zeros_like(w)
        wbd[...] = jnp.concatenate([jnp.concatenate([w, z], axis=1), jnp.concatenate([z, w], axis=1)], axis=0)

    rhs = jnp.concatenate([back_ref[0, :, 0].reshape(256, C), back_ref[0, :, 1].reshape(256, C)], axis=1)
    bias = bias_ref[...].astype(F32) * 0.5
    bias = jnp.concatenate([bias, bias], axis=1)
    c0 = np.float32(2.0 * np.sqrt(2.0 / np.pi))
    c1 = np.float32(8.0 * 0.044715 * np.sqrt(2.0 / np.pi))
    for i in range(4):
        lhs = jnp.concatenate([x_ref[i, 0], x_ref[i, 1]], axis=1)
        h = dot(lhs, wbd[...]) + dot(t6m[4 * xh + i], rhs) + bias
        o = h + h * jnp.tanh(h * (c0 + c1 * (h * h)))
        o = o.astype(BF)
        out_ref[i, 0] = o[:, :C]
        out_ref[i, 1] = o[:, C:]


def per_device(grid_features, weight_real, weight_imag, mode_keep, local_weight, local_bias):
    t1, t2, t3, t4, t5, t6 = tables()
    any_spec = pl.BlockSpec(memory_space=pl.ANY)
    vmem_spec = pl.BlockSpec(memory_space=pltpu.VMEM)
    V = lambda *s: pltpu.VMEM(s, BF)
    D = pltpu.SemaphoreType.DMA
    back = pl.pallas_call(
        spectral_kernel,
        out_shape=jax.ShapeDtypeStruct((4, NA, 4, 16, C), BF),
        in_specs=[any_spec] * 3 + [pl.BlockSpec(memory_space=pltpu.SMEM)] + [any_spec] * 5,
        out_specs=vmem_spec,
        scratch_shapes=[
            V(4, 8, 4, NZ, C), V(2, 4, KY, C, C), V(128, 256), V(4, 128, 256), V(256, 256), V(4, 256, 256),
            V(128, 256), V(1024, 256), V(512, 128),
            V(4, NA, 4, 16, C), V(4, NA, 4, 16, C), V(2, KX, 16, C), V(2, NB, 4, 16, C),
            V(2, NB, 4, 16, C), V(2, NB, 4, 16, C), V(4, NA, 4, 16, C),
            D((4,)), D((2,)), D((5,)), D(()), D((4,)), D(()), D((2,)), D(()), D((2,)), D(()), D((4,)),
        ],
        compiler_params=pltpu.CompilerParams(collective_id=0, has_side_effects=True, vmem_limit_bytes=40 << 20),
        name="spectral",
    )(grid_features, weight_real.reshape(4, KY, C, C), weight_imag.reshape(4, KY, C, C), mode_keep,
      jnp.asarray(t1), jnp.asarray(t2), jnp.asarray(t3), jnp.asarray(t4), jnp.asarray(t5))

    return pl.pallas_call(
        final_kernel,
        grid=(8, 2),
        out_shape=jax.ShapeDtypeStruct((8, 16, NZ, C), BF),
        in_specs=[
            pl.BlockSpec((4, 2, NZ, C), lambda j, x: (x, j, 0, 0)),
            pl.BlockSpec((1, NA, 2, 16, C), lambda j, x: (j // 2, 0, j % 2, 0, 0)),
            pl.BlockSpec((C, C), lambda j, x: (0, 0)),
            pl.BlockSpec((1, C), lambda j, x: (0, 0)),
            pl.BlockSpec((256, 256), lambda j, x: (0, 0)),
        ],
        out_specs=pl.BlockSpec((4, 2, NZ, C), lambda j, x: (x, j, 0, 0)),
        scratch_shapes=[V(8, 256, 256), V(256, 256)],
        compiler_params=pltpu.CompilerParams(vmem_limit_bytes=20 << 20),
        name="combine",
    )(grid_features, back, local_weight, local_bias.reshape(1, C), jnp.asarray(t6))


def solution(mesh):
    in_specs = (P("aa", "ba", None, None), P("ba", None, "aa", None, None), P("ba", None, "aa", None, None),
                P("ba", "aa"), P(), P())
    return jax.shard_map(per_device, mesh=mesh, in_specs=in_specs, out_specs=P("aa", "ba", None, None), check_vma=False)
```

```python
import numpy as np
import jax
import jax.numpy as jnp
from jax import lax
from jax.experimental import pallas as pl
from jax.experimental.pallas import tpu as pltpu
from jax.sharding import PartitionSpec as P

NX, NY, NZ, C = 128, 128, 256, 128
KX, KY, KZ = 32, 32, 16
NA, NB = 16, 8
MESH = pl.DeviceIdType.MESH
BF = jnp.bfloat16
F32 = jnp.float32

AA_ORDER = [(2, 2), (3, 2), (1, 2), (2, 3), (2, 1), (3, 1), (1, 3), (3, 3), (1, 1), (0, 2),
            (2, 0), (0, 3), (3, 0), (0, 1), (1, 0)]
BA_ORDER = [(2, 1), (2, 0), (1, 1), (3, 1), (1, 0), (3, 0), (0, 1)]


def kept(length, number):
    j = np.arange(number)
    return np.where(j < number // 2, j, j + length - number)


def angle(k, n, length):
    return 2.0 * np.pi * ((k * n) % length) / length


def complex_block(theta, ri_out, ri_in, sign):
    c, s = np.cos(theta), sign * np.sin(theta)
    return np.where(ri_out == ri_in, c, np.where(ri_out == 0, -s, s))


def tables():
    kx, ky = kept(NX, KX), kept(NY, KY)
    k, _, r, z = np.ix_(np.arange(KZ), np.arange(4), np.arange(2), np.arange(NZ))
    th = angle(k, z, NZ)
    t1 = np.where(r == 0, np.cos(th), -np.sin(th)) + np.zeros((KZ, 4, 2, NZ))
    t1 = t1.reshape(128, 256)
    k, _, r, x, q = np.ix_(kx, np.arange(2), np.arange(2), np.arange(NX), np.arange(2))
    t2 = complex_block(angle(k, x, NX), r, q, -1) + np.zeros((KX, 2, 2, NX, 2))
    t2 = t2.reshape(128, 256)
    k8, m, k4, r, g, b, yh, n, yl, q = np.ix_(*map(np.arange, (8, 2, 4, 2, 4, NB, 2, 2, 2, 2)))
    th = angle(ky[k8 * 4 + k4], b * 16 + g * 4 + yh * 2 + yl, NY)
    f = (complex_block(th, r, q, -1) * (m == n)).reshape(8, 2, 4, 2, 512)
    t3 = np.stack([f, np.stack([-f[:, :, :, 1], f[:, :, :, 0]], axis=3)]).reshape(256, 512)
    g, b, y, m, r, p, k8, n, k4, q = np.ix_(*map(np.arange, (4, NB, 4, 4, 2, 2, 8, 2, 4, 2)))
    t4 = complex_block(angle(ky[k8 * 4 + k4], b * 16 + g * 4 + y, NY), r, q, 1) * (m == 2 * p + n)
    t4 = t4.reshape(1024, 256)
    y, x, r, b, w, m, q = np.ix_(np.arange(2), np.arange(NX), np.arange(2), np.arange(NB), np.arange(2),
                                 np.arange(4), np.arange(2))
    t5 = complex_block(angle(kx[b * 4 + m], x, NX), r, q, 1) * (y == w)
    t5 = t5.reshape(512, 128)
    z, k, _, r = np.ix_(np.arange(NZ), np.arange(KZ), np.arange(8), np.arange(2))
    th = angle(k, z, NZ)
    t6 = np.where(r == 0, np.cos(th), -np.sin(th)) * np.where(k == 0, 1.0, 2.0) / (NX * NY * NZ) * 0.5
    t6 = (t6 + np.zeros((NZ, KZ, 8, 2))).reshape(256, 256)
    return [np.asarray(t, np.float32).astype(jnp.bfloat16) for t in (t1, t2, t3, t4, t5, t6)]


def dot(a, b):
    return jnp.dot(a, b, preferred_element_type=F32)


def bias_row(bias_ref):
    bias = bias_ref[...].astype(F32) * 0.5
    return jnp.concatenate([bias, bias], axis=1)


def back_pair(back_ref, y):
    return jnp.concatenate([back_ref[:, y].reshape(256, C), back_ref[:, y + 1].reshape(256, C)], axis=1)


def combine(first, second, weights, inverse, back, bias):
    c0 = np.float32(2.0 * np.sqrt(2.0 / np.pi))
    c1 = np.float32(8.0 * 0.044715 * np.sqrt(2.0 / np.pi))
    v = dot(jnp.concatenate([first, second], axis=1), weights) + dot(inverse, back) + bias
    return (v + v * jnp.tanh(v * (c0 + c1 * (v * v)))).astype(BF)


def spectral_kernel(x_hbm, wr_hbm, wi_hbm, keep_hbm, t1_hbm, t2_hbm, t3_hbm, t4_hbm, t5_hbm, t6_hbm, w_hbm, bias_hbm,
                    out_ref, xlast, blast, t6m, wbd,
                    xv, wv, keep_ref, t1v, t1m, t2v, t2m, t3v, t4v, t5v, t6v, lw, bias_ref, s1, r1, s2, r2, s3, r3, s4, r4,
                    xsem, wsem, tsem, sa, ra, sb, rb, sc, rc, sd, rd):
    ia, ib = lax.axis_index("aa"), lax.axis_index("ba")
    ix, iz, iy, ic = ia // 4, lax.rem(ia, 4), ib // 2, lax.rem(ib, 2)
    aa_peers = [lax.rem(ix + dx, 4) * 4 + lax.rem(iz + dz, 4) for dx, dz in AA_ORDER]
    ba_peers = [lax.rem(iy + dy, 4) * 2 + lax.rem(ic + dc, 2) for dy, dc in BA_ORDER]

    tcopies = [pltpu.make_async_copy(src, dst, tsem.at[i]) for i, (src, dst) in enumerate(
        [(t1_hbm, t1v), (t2_hbm, t2v), (t3_hbm, t3v), (t4_hbm, t4v), (t5_hbm, t5v), (t6_hbm, t6v), (w_hbm, lw), (bias_hbm, bias_ref)])]
    tcopies[0].start()
    xg = [xv.at[0], xv.at[1], xv.at[2], xlast]
    xcopies = [pltpu.make_async_copy(x_hbm.at[:, pl.ds(4 * g, 4)], xg[g], xsem.at[g]) for g in range(4)]
    for c in xcopies:
        c.start()
    tcopies[1].start()
    wcopies = [pltpu.make_async_copy(wr_hbm, wv.at[0], wsem.at[0]), pltpu.make_async_copy(wi_hbm, wv.at[1], wsem.at[1]),
               pltpu.make_async_copy(keep_hbm, keep_ref, wsem.at[2])]

    barrier = pltpu.get_barrier_semaphore()
    for t in aa_peers:
        pl.semaphore_signal(barrier, inc=1, device_id={"aa": t}, device_id_type=MESH)
    for t in ba_peers:
        pl.semaphore_signal(barrier, inc=1, device_id={"ba": t}, device_id_type=MESH)

    def send_aa(src, dst, ssem, rsem):
        for t in aa_peers:
            pltpu.make_async_remote_copy(src.at[t], dst.at[ia], ssem, rsem, device_id={"aa": t}, device_id_type=MESH).start()

    def send_ba(src, dst, ssem, rsem):
        for t in ba_peers:
            pltpu.make_async_remote_copy(src(t), dst.at[ib], ssem, rsem, device_id={"ba": t}, device_id_type=MESH).start()

    def wait_bytes(ref, sem):
        pltpu.make_async_copy(ref, ref, sem).wait()

    tcopies[0].wait()
    rows1 = lax.broadcasted_iota(jnp.int32, (128, 256), 0) // 2 % 4
    for i in range(4):
        t1m[i] = jnp.where(rows1 == i, t1v[...].astype(F32), 0.0).astype(BF)
    for g in range(4):
        xcopies[g].wait()
        for y in range(4):
            acc = None
            for i in range(4):
                rhs = jnp.concatenate([xg[g][i, y], xg[g][i + 4, y]], axis=1)
                p = dot(t1m[i], rhs)
                acc = p if acc is None else acc + p
            acc = acc.reshape(KZ, 8, 256)
            s1[g, :, y] = jnp.concatenate([acc[:, :, :128], acc[:, :, 128:]], axis=1).astype(BF)
        if g == 0:
            pl.semaphore_wait(barrier, len(aa_peers) + len(ba_peers))
        send_aa(s1.at[g], r1.at[g], sa, ra.at[g])
        r1[g, ia] = s1[g, ia]

    for c in tcopies[2:] + wcopies:
        c.start()
    tcopies[1].wait()
    rows2 = lax.broadcasted_iota(jnp.int32, (128, 256), 0) // 2 % 2
    for i in range(2):
        t2m[i] = jnp.where(rows2 == i, t2v[...].astype(F32), 0.0).astype(BF)
    for c in tcopies[2:]:
        c.wait()
    lanes6 = lax.broadcasted_iota(jnp.int32, (256, 256), 1) // 2 % 8
    for i in range(8):
        t6m[i] = jnp.where(lanes6 == i, t6v[...].astype(F32), 0.0).astype(BF)
    half_w = (lw[...].astype(F32) * 0.5).astype(BF)
    zero_w = jnp.zeros_like(half_w)
    wbd[...] = jnp.concatenate([jnp.concatenate([half_w, zero_w], axis=1), jnp.concatenate([zero_w, half_w], axis=1)], axis=0)

    for g in range(4):
        wait_bytes(r1.at[g, pl.ds(0, NA - 1)], ra.at[g])
        acc = None
        for i in range(2):
            rhs = jnp.concatenate([r1[g, :, i].reshape(256, C), r1[g, :, i + 2].reshape(256, C)], axis=1)
            p = dot(t2m[i], rhs)
            acc = p if acc is None else acc + p
        acc = acc.reshape(KX // 2, 8, 256)
        s2[g] = jnp.concatenate([acc[:, :, :C], acc[:, :, C:]], axis=1).astype(BF)
        send_ba(lambda t: s2.at[g, pl.ds(2 * t, 2)], r2.at[g], sb, rb.at[g])
        r2[g, ib] = s2[g, pl.ds(2 * ib, 2)]

    for c in wcopies:
        c.wait()
    for g in range(4):
        wait_bytes(r2.at[g, pl.ds(0, NB - 1)], rb.at[g])

    block = lax.broadcasted_iota(jnp.int32, (16, 256), 0) // 2 % 4
    row = lax.broadcasted_iota(jnp.int32, (16, C), 0)
    mixed = []
    for p in range(2):
        spec = dot(t3v[...], r2[:, :, p].reshape(512, C))
        keep = jnp.where(row < 8, keep_ref[0, 2 * p], keep_ref[0, 2 * p + 1])
        for q in range(8):
            lhs = jnp.concatenate([spec[16 * q:16 * q + 16], spec[128 + 16 * q:128 + 16 * q + 16]], axis=1)
            acc = None
            for j in range(4):
                k = 4 * q + j
                w = jnp.concatenate([jnp.concatenate([wv[r, 2 * p, k], wv[r, 2 * p + 1, k]], axis=1) for r in range(2)], axis=0)
                part = dot(jnp.where(block == j, lhs, 0.0).astype(BF), w)
                acc = part if acc is None else acc + part
            position = 4 * q + row // 2 % 4
            level = jnp.where(position < KY // 2, position, KY - 1 - position)
            mixed.append(jnp.where(level < keep, jnp.where(row < 8, acc[:, :C], acc[:, C:]), 0.0))
    rhs = jnp.concatenate(mixed, axis=0).astype(BF)
    for g in range(4):
        s3[g] = dot(t4v[pl.ds(256 * g, 256)], rhs).astype(BF).reshape(NB, 2, 16, C)
        send_ba(lambda t: s3.at[g, t], r3.at[g], sc, rc.at[g])
        r3[g, ib] = s3[g, ib]

    for g in range(4):
        wait_bytes(r3.at[g, pl.ds(0, NB - 1)], rc.at[g])
        rhs = jnp.concatenate([r3[g, :, 0].reshape(128, C), r3[g, :, 1].reshape(128, C)], axis=1)
        for i in range(2):
            back = dot(t5v[pl.ds(256 * i, 256)], rhs).astype(BF)
            for half in range(2):
                s4[g, :, 2 * half + i] = back[:, C * half:C * half + C].reshape(NA, 16, C)
        land = r4.at[g] if g < 3 else blast
        send_aa(s4.at[g], land, sd, rd.at[g])
        land[ia] = s4[g, ia]

    bias = bias_row(bias_ref)
    for g in range(3):
        wait_bytes(r4.at[g, pl.ds(0, NA - 1)], rd.at[g])
        for y in (0, 2):
            rhs = back_pair(r4.at[g], y)
            for x in range(8):
                o = combine(xv[g, x, y], xv[g, x, y + 1], wbd[...], t6m[x], rhs, bias)
                out_ref[x, 4 * g + y] = o[:, :C]
                out_ref[x, 4 * g + y + 1] = o[:, C:]

    wait_bytes(blast.at[pl.ds(0, NA - 1)], rd.at[3])
    wait_bytes(s1.at[:, pl.ds(0, NA - 1)], sa)
    wait_bytes(s4.at[:, pl.ds(0, NA - 1)], sd)
    wait_bytes(r2.at[:, pl.ds(0, NB - 1)], sb)
    wait_bytes(r3.at[:, pl.ds(0, NB - 1)], sc)


def store_kernel(val_ref, xlast, blast, t6m, wbd, bias_ref, out_ref, tail, sem):
    copies = [pltpu.make_async_copy(val_ref.at[i], out_ref.at[i, pl.ds(0, 12)], sem.at[i]) for i in range(8)]
    tails = [pltpu.make_async_copy(tail.at[i], out_ref.at[i, pl.ds(12, 4)], sem.at[8 + i]) for i in range(8)]
    for c in copies:
        c.start()
    bias = bias_row(bias_ref)
    rhs = [back_pair(blast, y) for y in (0, 2)]
    for x in range(8):
        for i in range(2):
            o = combine(xlast[x, 2 * i], xlast[x, 2 * i + 1], wbd[...], t6m[x], rhs[i], bias)
            tail[x, 2 * i] = o[:, :C]
            tail[x, 2 * i + 1] = o[:, C:]
        if x > 0:
            tails[x - 1].start()
    tails[7].start()
    for c in copies + tails:
        c.wait()


def per_device(grid_features, weight_real, weight_imag, mode_keep, local_weight, local_bias):
    t1, t2, t3, t4, t5, t6 = tables()
    any_spec = pl.BlockSpec(memory_space=pltpu.HBM)
    vmem_spec = pl.BlockSpec(memory_space=pltpu.VMEM)
    V = lambda *s: pltpu.VMEM(s, BF)
    D = pltpu.SemaphoreType.DMA
    hbm = lambda a: pltpu.with_memory_space_constraint(a, pltpu.HBM)
    results = pl.pallas_call(
        spectral_kernel,
        out_shape=[jax.ShapeDtypeStruct(shape, BF) for shape in (
            (8, 12, NZ, C), (8, 4, NZ, C), (NA, 4, 16, C), (8, 256, 256), (256, 256))],
        in_specs=[any_spec] * 12,
        out_specs=[vmem_spec] * 5,
        scratch_shapes=[
            V(3, 8, 4, NZ, C), V(2, 4, KY, C, C), pltpu.SMEM((1, 4), jnp.int32), V(128, 256), V(4, 128, 256),
            V(128, 256), V(2, 128, 256), V(256, 512), V(1024, 256), V(512, 128), V(256, 256), V(C, C), V(1, C),
            V(4, NA, 4, 16, C), V(4, NA, 4, 16, C), V(4, KX // 2, 16, C), V(4, NB, 2, 16, C),
            V(4, NB, 2, 16, C), V(4, NB, 2, 16, C), V(4, NA, 4, 16, C), V(3, NA, 4, 16, C),
            D((4,)), D((3,)), D((8,)), D(()), D((4,)), D(()), D((4,)), D(()), D((4,)), D(()), D((4,)),
        ],
        compiler_params=pltpu.CompilerParams(collective_id=0, has_side_effects=True, vmem_limit_bytes=40 << 20),
        name="spectral",
    )(*map(hbm, (grid_features, weight_real.reshape(4, KY, C, C), weight_imag.reshape(4, KY, C, C), mode_keep.reshape(1, 4),
                 *map(jnp.asarray, (t1, t2, t3, t4, t5, t6)), local_weight, local_bias.reshape(1, C))))

    return pl.pallas_call(
        store_kernel,
        out_shape=jax.ShapeDtypeStruct((8, 16, NZ, C), BF),
        in_specs=[vmem_spec] * 6,
        out_specs=any_spec,
        scratch_shapes=[V(8, 4, NZ, C), D((16,))],
        compiler_params=pltpu.CompilerParams(vmem_limit_bytes=6 << 20),
        name="store",
    )(*results, local_bias.reshape(1, C))


def solution(mesh):
    in_specs = (P("aa", "ba", None, None), P("ba", None, "aa", None, None), P("ba", None, "aa", None, None),
                P("ba", "aa"), P(), P())
    return jax.shard_map(per_device, mesh=mesh, in_specs=in_specs, out_specs=P("aa", "ba", None, None), check_vma=False)
```

```python
import numpy as np
import jax
import jax.numpy as jnp
from jax import lax
from jax.experimental import pallas as pl
from jax.experimental.pallas import tpu as pltpu
from jax.sharding import PartitionSpec as P

NX, NY, NZ, C = 128, 128, 256, 128
KX, KY, KZ = 32, 32, 16
NA, NB = 16, 8
MESH = pl.DeviceIdType.MESH
BF = jnp.bfloat16
F32 = jnp.float32

AA_ORDER = [(2, 2), (3, 2), (1, 2), (2, 3), (2, 1), (3, 1), (1, 3), (3, 3), (1, 1), (0, 2),
            (2, 0), (0, 3), (3, 0), (0, 1), (1, 0)]
EARLY_FIRST = [0, 1, 3, 4, 12, 2, 5, 7, 8, 13, 15, 6, 9, 11, 14, 10]
BA_ORDER = [(2, 1), (2, 0), (1, 1), (3, 1), (1, 0), (3, 0), (0, 1)]


def kept(length, number):
    j = np.arange(number)
    return np.where(j < number // 2, j, j + length - number)


def angle(k, n, length):
    return 2.0 * np.pi * ((k * n) % length) / length


def complex_block(theta, ri_out, ri_in, sign):
    c, s = np.cos(theta), sign * np.sin(theta)
    return np.where(ri_out == ri_in, c, np.where(ri_out == 0, -s, s))


def tables():
    kx, ky = kept(NX, KX), kept(NY, KY)
    k, _, r, z = np.ix_(np.arange(KZ), np.arange(4), np.arange(2), np.arange(NZ))
    th = angle(k, z, NZ)
    t1 = np.where(r == 0, np.cos(th), -np.sin(th)) + np.zeros((KZ, 4, 2, NZ))
    t1 = t1.reshape(128, 256)
    k, _, r, x, q = np.ix_(kx, np.arange(2), np.arange(2), np.arange(NX), np.arange(2))
    t2 = complex_block(angle(k, x, NX), r, q, -1) + np.zeros((KX, 2, 2, NX, 2))
    t2 = t2.reshape(128, 256)
    k8, m, k4, r, g, b, yh, n, yl, q = np.ix_(*map(np.arange, (8, 2, 4, 2, 4, NB, 2, 2, 2, 2)))
    th = angle(ky[k8 * 4 + k4], b * 16 + g * 4 + yh * 2 + yl, NY)
    f = (complex_block(th, r, q, -1) * (m == n)).reshape(8, 2, 4, 2, 512)
    t3 = np.stack([f, np.stack([-f[:, :, :, 1], f[:, :, :, 0]], axis=3)]).reshape(256, 512)
    g, b, y, m, r, p, k8, n, k4, q = np.ix_(*map(np.arange, (4, NB, 4, 4, 2, 2, 8, 2, 4, 2)))
    t4 = complex_block(angle(ky[k8 * 4 + k4], b * 16 + g * 4 + y, NY), r, q, 1) * (m == 2 * p + n)
    t4 = t4.reshape(1024, 256)
    y, x, r, b, w, m, q = np.ix_(np.arange(2), np.arange(NX), np.arange(2), np.arange(NB), np.arange(2),
                                 np.arange(4), np.arange(2))
    t5 = complex_block(angle(kx[b * 4 + m], x, NX), r, q, 1) * (y == w)
    t5 = t5.reshape(512, 128)
    z, k, _, r = np.ix_(np.arange(NZ), np.arange(KZ), np.arange(8), np.arange(2))
    th = angle(k, z, NZ)
    t6 = np.where(r == 0, np.cos(th), -np.sin(th)) * np.where(k == 0, 1.0, 2.0) / (NX * NY * NZ) * 0.5
    t6 = (t6 + np.zeros((NZ, KZ, 8, 2))).reshape(256, 256)
    return [np.asarray(t, np.float32).astype(jnp.bfloat16) for t in (t1, t2, t3, t4, t5, t6)]


def dot(a, b):
    return jnp.dot(a, b, preferred_element_type=F32)


def bias_row(bias_ref):
    bias = bias_ref[...].astype(F32) * 0.5
    return jnp.concatenate([bias, bias], axis=1)


def back_pair(back_ref, y):
    return jnp.concatenate([back_ref[:, y].reshape(256, C), back_ref[:, y + 1].reshape(256, C)], axis=1)


def combine(first, second, weights, inverse, back, bias):
    c0 = np.float32(2.0 * np.sqrt(2.0 / np.pi))
    c1 = np.float32(8.0 * 0.044715 * np.sqrt(2.0 / np.pi))
    v = dot(jnp.concatenate([first, second], axis=1), weights) + dot(inverse, back) + bias
    return (v + v * jnp.tanh(v * (c0 + c1 * (v * v)))).astype(BF)


def spectral_kernel(x_hbm, wr_hbm, wi_hbm, keep_hbm, t1_hbm, t2_hbm, t3_hbm, t4_hbm, t5_hbm, t6_hbm, w_hbm, bias_hbm,
                    out_ref, xlast, blast, t6m, wbd,
                    xv, wv, keep_ref, t1v, t1m, t2v, t2m, t3v, t4v, t5v, t6v, lw, bias_ref, s1, r1, s2, r2, s3, r3, s4, r4,
                    xsem, wsem, tsem, sa, ra, sb, rb, sc, rc, sd, rd):
    ia, ib = lax.axis_index("aa"), lax.axis_index("ba")
    ix, iz, iy, ic = ia // 4, lax.rem(ia, 4), ib // 2, lax.rem(ib, 2)
    aa_peers = [lax.rem(ix + dx, 4) * 4 + lax.rem(iz + dz, 4) for dx, dz in AA_ORDER]
    ba_peers = [lax.rem(iy + dy, 4) * 2 + lax.rem(ic + dc, 2) for dy, dc in BA_ORDER]

    tcopies = [pltpu.make_async_copy(src, dst, tsem.at[i]) for i, (src, dst) in enumerate(
        [(t1_hbm, t1v), (t2_hbm, t2v), (t3_hbm, t3v), (t4_hbm, t4v), (t5_hbm, t5v), (t6_hbm, t6v), (w_hbm, lw), (bias_hbm, bias_ref)])]
    tcopies[0].start()
    xg = [xv.at[0], xv.at[1], xv.at[2], xlast]
    xcopies = [pltpu.make_async_copy(x_hbm.at[:, pl.ds(4 * g, 4)], xg[g], xsem.at[g]) for g in range(4)]
    for c in xcopies:
        c.start()
    tcopies[1].start()
    wcopies = [pltpu.make_async_copy(wr_hbm, wv.at[0], wsem.at[0]), pltpu.make_async_copy(wi_hbm, wv.at[1], wsem.at[1]),
               pltpu.make_async_copy(keep_hbm, keep_ref, wsem.at[2])]

    barrier = pltpu.get_barrier_semaphore()
    for t in aa_peers:
        pl.semaphore_signal(barrier, inc=1, device_id={"aa": t}, device_id_type=MESH)
    for t in ba_peers:
        pl.semaphore_signal(barrier, inc=1, device_id={"ba": t}, device_id_type=MESH)

    def send_aa(src, dst, ssem, rsem):
        for t in aa_peers:
            pltpu.make_async_remote_copy(src.at[t], dst.at[ia], ssem, rsem, device_id={"aa": t}, device_id_type=MESH).start()

    def send_ba(src, dst, ssem, rsem):
        for t in ba_peers:
            pltpu.make_async_remote_copy(src(t), dst.at[ib], ssem, rsem, device_id={"ba": t}, device_id_type=MESH).start()

    def wait_bytes(ref, sem):
        pltpu.make_async_copy(ref, ref, sem).wait()

    tcopies[0].wait()
    rows1 = lax.broadcasted_iota(jnp.int32, (128, 256), 0) // 2 % 4
    for i in range(4):
        t1m[i] = jnp.where(rows1 == i, t1v[...].astype(F32), 0.0).astype(BF)
    for g in range(4):
        xcopies[g].wait()
        for y in range(4):
            acc = None
            for i in range(4):
                rhs = jnp.concatenate([xg[g][i, y], xg[g][i + 4, y]], axis=1)
                p = dot(t1m[i], rhs)
                acc = p if acc is None else acc + p
            acc = acc.reshape(KZ, 8, 256)
            s1[g, :, y] = jnp.concatenate([acc[:, :, :128], acc[:, :, 128:]], axis=1).astype(BF)
        if g == 0:
            pl.semaphore_wait(barrier, len(aa_peers) + len(ba_peers))
        send_aa(s1.at[g], r1.at[g], sa, ra.at[g])
        r1[g, ia] = s1[g, ia]

    for c in tcopies[2:] + wcopies:
        c.start()
    tcopies[1].wait()
    rows2 = lax.broadcasted_iota(jnp.int32, (128, 256), 0) // 2 % 2
    for i in range(2):
        t2m[i] = jnp.where(rows2 == i, t2v[...].astype(F32), 0.0).astype(BF)
    for c in tcopies[2:]:
        c.wait()
    lanes6 = lax.broadcasted_iota(jnp.int32, (256, 256), 1) // 2 % 8
    for i in range(8):
        t6m[i] = jnp.where(lanes6 == i, t6v[...].astype(F32), 0.0).astype(BF)
    half_w = (lw[...].astype(F32) * 0.5).astype(BF)
    zero_w = jnp.zeros_like(half_w)
    wbd[...] = jnp.concatenate([jnp.concatenate([half_w, zero_w], axis=1), jnp.concatenate([zero_w, half_w], axis=1)], axis=0)

    for g in range(4):
        wait_bytes(r1.at[g, pl.ds(0, NA - 1)], ra.at[g])
        acc = None
        for i in range(2):
            rhs = jnp.concatenate([r1[g, :, i].reshape(256, C), r1[g, :, i + 2].reshape(256, C)], axis=1)
            p = dot(t2m[i], rhs)
            acc = p if acc is None else acc + p
        acc = acc.reshape(KX // 2, 8, 256)
        s2[g] = jnp.concatenate([acc[:, :, :C], acc[:, :, C:]], axis=1).astype(BF)
        send_ba(lambda t: s2.at[g, pl.ds(2 * t, 2)], r2.at[g], sb, rb.at[g])
        r2[g, ib] = s2[g, pl.ds(2 * ib, 2)]

    for c in wcopies:
        c.wait()
    for g in range(4):
        wait_bytes(r2.at[g, pl.ds(0, NB - 1)], rb.at[g])

    block = lax.broadcasted_iota(jnp.int32, (16, 256), 0) // 2 % 4
    row = lax.broadcasted_iota(jnp.int32, (16, C), 0)
    mixed = []
    for p in range(2):
        spec = dot(t3v[...], r2[:, :, p].reshape(512, C))
        keep = jnp.where(row < 8, keep_ref[0, 2 * p], keep_ref[0, 2 * p + 1])
        for q in range(8):
            lhs = jnp.concatenate([spec[16 * q:16 * q + 16], spec[128 + 16 * q:128 + 16 * q + 16]], axis=1)
            acc = None
            for j in range(4):
                k = 4 * q + j
                w = jnp.concatenate([jnp.concatenate([wv[r, 2 * p, k], wv[r, 2 * p + 1, k]], axis=1) for r in range(2)], axis=0)
                part = dot(jnp.where(block == j, lhs, 0.0).astype(BF), w)
                acc = part if acc is None else acc + part
            position = 4 * q + row // 2 % 4
            level = jnp.where(position < KY // 2, position, KY - 1 - position)
            mixed.append(jnp.where(level < keep, jnp.where(row < 8, acc[:, :C], acc[:, C:]), 0.0))
    rhs = jnp.concatenate(mixed, axis=0).astype(BF)
    for g in range(4):
        s3[g] = dot(t4v[pl.ds(256 * g, 256)], rhs).astype(BF).reshape(NB, 2, 16, C)
        send_ba(lambda t: s3.at[g, t], r3.at[g], sc, rc.at[g])
        r3[g, ib] = s3[g, ib]

    for g in range(4):
        wait_bytes(r3.at[g, pl.ds(0, NB - 1)], rc.at[g])
        rhs = jnp.concatenate([r3[g, :, 0].reshape(128, C), r3[g, :, 1].reshape(128, C)], axis=1)
        for i in range(2):
            back = dot(t5v[pl.ds(256 * i, 256)], rhs).astype(BF)
            for half in range(2):
                s4[g, :, 2 * half + i] = back[:, C * half:C * half + C].reshape(NA, 16, C)
        land = r4.at[g] if g < 3 else blast
        if g == 3:
            for t in EARLY_FIRST:
                @pl.when(ia != t)
                def _():
                    pltpu.make_async_remote_copy(s4.at[g, t], land.at[ia], sd, rd.at[g], device_id={"aa": t}, device_id_type=MESH).start()
        else:
            send_aa(s4.at[g], land, sd, rd.at[g])
        land[ia] = s4[g, ia]

    bias = bias_row(bias_ref)
    for g in range(3):
        wait_bytes(r4.at[g, pl.ds(0, NA - 1)], rd.at[g])
        for y in (0, 2):
            rhs = back_pair(r4.at[g], y)
            for x in range(8):
                o = combine(xv[g, x, y], xv[g, x, y + 1], wbd[...], t6m[x], rhs, bias)
                out_ref[x, 4 * g + y] = o[:, :C]
                out_ref[x, 4 * g + y + 1] = o[:, C:]

    wait_bytes(blast.at[pl.ds(0, NA - 1)], rd.at[3])
    wait_bytes(s1.at[:, pl.ds(0, NA - 1)], sa)
    wait_bytes(s4.at[:, pl.ds(0, NA - 1)], sd)
    wait_bytes(r2.at[:, pl.ds(0, NB - 1)], sb)
    wait_bytes(r3.at[:, pl.ds(0, NB - 1)], sc)


def store_kernel(val_ref, xlast, blast, t6m, wbd, bias_ref, out_ref, tail, sem):
    copies = [pltpu.make_async_copy(val_ref.at[i], out_ref.at[i, pl.ds(0, 12)], sem.at[i]) for i in range(8)]
    tails = [pltpu.make_async_copy(tail.at[i], out_ref.at[i, pl.ds(12, 4)], sem.at[8 + i]) for i in range(8)]
    for c in copies:
        c.start()
    bias = bias_row(bias_ref)
    rhs = [back_pair(blast, y) for y in (0, 2)]
    for x in range(8):
        for i in range(2):
            o = combine(xlast[x, 2 * i], xlast[x, 2 * i + 1], wbd[...], t6m[x], rhs[i], bias)
            tail[x, 2 * i] = o[:, :C]
            tail[x, 2 * i + 1] = o[:, C:]
        if x > 0:
            tails[x - 1].start()
    tails[7].start()
    for c in copies + tails:
        c.wait()


def per_device(grid_features, weight_real, weight_imag, mode_keep, local_weight, local_bias):
    t1, t2, t3, t4, t5, t6 = tables()
    any_spec = pl.BlockSpec(memory_space=pltpu.HBM)
    vmem_spec = pl.BlockSpec(memory_space=pltpu.VMEM)
    V = lambda *s: pltpu.VMEM(s, BF)
    D = pltpu.SemaphoreType.DMA
    hbm = lambda a: pltpu.with_memory_space_constraint(a, pltpu.HBM)
    results = pl.pallas_call(
        spectral_kernel,
        out_shape=[jax.ShapeDtypeStruct(shape, BF) for shape in (
            (8, 12, NZ, C), (8, 4, NZ, C), (NA, 4, 16, C), (8, 256, 256), (256, 256))],
        in_specs=[any_spec] * 12,
        out_specs=[vmem_spec] * 5,
        scratch_shapes=[
            V(3, 8, 4, NZ, C), V(2, 4, KY, C, C), pltpu.SMEM((1, 4), jnp.int32), V(128, 256), V(4, 128, 256),
            V(128, 256), V(2, 128, 256), V(256, 512), V(1024, 256), V(512, 128), V(256, 256), V(C, C), V(1, C),
            V(4, NA, 4, 16, C), V(4, NA, 4, 16, C), V(4, KX // 2, 16, C), V(4, NB, 2, 16, C),
            V(4, NB, 2, 16, C), V(4, NB, 2, 16, C), V(4, NA, 4, 16, C), V(3, NA, 4, 16, C),
            D((4,)), D((3,)), D((8,)), D(()), D((4,)), D(()), D((4,)), D(()), D((4,)), D(()), D((4,)),
        ],
        compiler_params=pltpu.CompilerParams(collective_id=0, has_side_effects=True, vmem_limit_bytes=40 << 20),
        name="spectral",
    )(*map(hbm, (grid_features, weight_real.reshape(4, KY, C, C), weight_imag.reshape(4, KY, C, C), mode_keep.reshape(1, 4),
                 *map(jnp.asarray, (t1, t2, t3, t4, t5, t6)), local_weight, local_bias.reshape(1, C))))

    return pl.pallas_call(
        store_kernel,
        out_shape=jax.ShapeDtypeStruct((8, 16, NZ, C), BF),
        in_specs=[vmem_spec] * 6,
        out_specs=any_spec,
        scratch_shapes=[V(8, 4, NZ, C), D((16,))],
        compiler_params=pltpu.CompilerParams(vmem_limit_bytes=6 << 20),
        name="store",
    )(*results, local_bias.reshape(1, C))


def solution(mesh):
    in_specs = (P("aa", "ba", None, None), P("ba", None, "aa", None, None), P("ba", None, "aa", None, None),
                P("ba", "aa"), P(), P())
    return jax.shard_map(per_device, mesh=mesh, in_specs=in_specs, out_specs=P("aa", "ba", None, None), check_vma=False)
```

```python
import numpy as np
import jax
import jax.numpy as jnp
from jax import lax
from jax.experimental import pallas as pl
from jax.experimental.pallas import tpu as pltpu
from jax.sharding import PartitionSpec as P

NX, NY, NZ, C = 128, 128, 256, 128
KX, KY, KZ = 32, 32, 16
NA, NB = 16, 8
MESH = pl.DeviceIdType.MESH
BF = jnp.bfloat16
F32 = jnp.float32

AA_ORDER = [(2, 2), (3, 2), (1, 2), (2, 3), (2, 1), (3, 1), (1, 3), (3, 3), (1, 1), (0, 2),
            (2, 0), (0, 3), (3, 0), (0, 1), (1, 0)]
EARLY_FIRST = [0, 1, 3, 4, 12, 2, 5, 7, 8, 13, 15, 6, 9, 11, 14, 10]
BA_ORDER = [(2, 1), (2, 0), (1, 1), (3, 1), (1, 0), (3, 0), (0, 1)]


def kept(length, number):
    j = np.arange(number)
    return np.where(j < number // 2, j, j + length - number)


def angle(k, n, length):
    return 2.0 * np.pi * ((k * n) % length) / length


def complex_block(theta, ri_out, ri_in, sign):
    c, s = np.cos(theta), sign * np.sin(theta)
    return np.where(ri_out == ri_in, c, np.where(ri_out == 0, -s, s))


def tables():
    kx, ky = kept(NX, KX), kept(NY, KY)
    k, _, r, z = np.ix_(np.arange(KZ), np.arange(4), np.arange(2), np.arange(NZ))
    th = angle(k, z, NZ)
    t1 = np.where(r == 0, np.cos(th), -np.sin(th)) + np.zeros((KZ, 4, 2, NZ))
    t1 = t1.reshape(128, 256)
    k, _, r, x, q = np.ix_(kx, np.arange(2), np.arange(2), np.arange(NX), np.arange(2))
    t2 = complex_block(angle(k, x, NX), r, q, -1) + np.zeros((KX, 2, 2, NX, 2))
    t2 = t2.reshape(128, 256)
    k8, m, k4, r, g, b, yh, n, yl, q = np.ix_(*map(np.arange, (8, 2, 4, 2, 4, NB, 2, 2, 2, 2)))
    th = angle(ky[k8 * 4 + k4], b * 16 + g * 4 + yh * 2 + yl, NY)
    f = (complex_block(th, r, q, -1) * (m == n)).reshape(8, 2, 4, 2, 512)
    t3 = np.stack([f, np.stack([-f[:, :, :, 1], f[:, :, :, 0]], axis=3)]).reshape(256, 512)
    g, b, y, m, r, p, k8, n, k4, q = np.ix_(*map(np.arange, (8, NB, 2, 4, 2, 2, 8, 2, 4, 2)))
    t4 = complex_block(angle(ky[k8 * 4 + k4], b * 16 + g * 2 + y, NY), r, q, 1) * (m == 2 * p + n)
    t4 = t4.reshape(1024, 256)
    y, x, r, b, w, m, q = np.ix_(np.arange(2), np.arange(NX), np.arange(2), np.arange(NB), np.arange(2),
                                 np.arange(4), np.arange(2))
    t5 = complex_block(angle(kx[b * 4 + m], x, NX), r, q, 1) * (y == w)
    t5 = t5.reshape(512, 128)
    z, k, _, r = np.ix_(np.arange(NZ), np.arange(KZ), np.arange(8), np.arange(2))
    th = angle(k, z, NZ)
    t6 = np.where(r == 0, np.cos(th), -np.sin(th)) * np.where(k == 0, 1.0, 2.0) / (NX * NY * NZ) * 0.5
    t6 = (t6 + np.zeros((NZ, KZ, 8, 2))).reshape(256, 256)
    return [np.asarray(t, np.float32).astype(jnp.bfloat16) for t in (t1, t2, t3, t4, t5, t6)]


def dot(a, b):
    return jnp.dot(a, b, preferred_element_type=F32)


def bias_row(bias_ref):
    bias = bias_ref[...].astype(F32) * 0.5
    return jnp.concatenate([bias, bias], axis=1)


def back_pair(back_ref, y):
    return jnp.concatenate([back_ref[:, y].reshape(256, C), back_ref[:, y + 1].reshape(256, C)], axis=1)


def combine(first, second, weights, inverse, back, bias):
    c0 = np.float32(2.0 * np.sqrt(2.0 / np.pi))
    c1 = np.float32(8.0 * 0.044715 * np.sqrt(2.0 / np.pi))
    v = dot(jnp.concatenate([first, second], axis=1), weights) + dot(inverse, back) + bias
    return (v + v * jnp.tanh(v * (c0 + c1 * (v * v)))).astype(BF)


def spectral_kernel(x_hbm, wr_hbm, wi_hbm, keep_hbm, t1_hbm, t2_hbm, t3_hbm, t4_hbm, t5_hbm, t6_hbm, w_hbm, bias_hbm,
                    out_ref, xlast, blast, t6m, wbd,
                    xv, wv, keep_ref, t1v, t1m, t2v, t2m, t3v, t4v, t5v, t6v, lw, bias_ref, s1, r1, s2, r2, s3, r3, s4, r4,
                    xsem, wsem, tsem, sa, ra, sb, rb, sc, rc, sd, rd):
    ia, ib = lax.axis_index("aa"), lax.axis_index("ba")
    ix, iz, iy, ic = ia // 4, lax.rem(ia, 4), ib // 2, lax.rem(ib, 2)
    aa_peers = [lax.rem(ix + dx, 4) * 4 + lax.rem(iz + dz, 4) for dx, dz in AA_ORDER]
    ba_peers = [lax.rem(iy + dy, 4) * 2 + lax.rem(ic + dc, 2) for dy, dc in BA_ORDER]

    tcopies = [pltpu.make_async_copy(src, dst, tsem.at[i]) for i, (src, dst) in enumerate(
        [(t1_hbm, t1v), (t2_hbm, t2v), (t3_hbm, t3v), (t4_hbm, t4v), (t5_hbm, t5v), (t6_hbm, t6v), (w_hbm, lw), (bias_hbm, bias_ref)])]
    tcopies[0].start()
    xg = [xv.at[0], xv.at[1], xv.at[2], xlast]
    xcopies = [pltpu.make_async_copy(x_hbm.at[:, pl.ds(4 * g, 4)], xg[g], xsem.at[g]) for g in range(4)]
    for c in xcopies:
        c.start()
    tcopies[1].start()
    wcopies = [pltpu.make_async_copy(wr_hbm, wv.at[0], wsem.at[0]), pltpu.make_async_copy(wi_hbm, wv.at[1], wsem.at[1]),
               pltpu.make_async_copy(keep_hbm, keep_ref, wsem.at[2])]

    barrier = pltpu.get_barrier_semaphore()
    for t in aa_peers:
        pl.semaphore_signal(barrier, inc=1, device_id={"aa": t}, device_id_type=MESH)
    for t in ba_peers:
        pl.semaphore_signal(barrier, inc=1, device_id={"ba": t}, device_id_type=MESH)

    def send_aa(src, dst, ssem, rsem):
        for t in aa_peers:
            pltpu.make_async_remote_copy(src.at[t], dst.at[ia], ssem, rsem, device_id={"aa": t}, device_id_type=MESH).start()

    def send_ba(src, dst, ssem, rsem):
        for t in ba_peers:
            pltpu.make_async_remote_copy(src(t), dst.at[ib], ssem, rsem, device_id={"ba": t}, device_id_type=MESH).start()

    def wait_bytes(ref, sem):
        pltpu.make_async_copy(ref, ref, sem).wait()

    tcopies[0].wait()
    rows1 = lax.broadcasted_iota(jnp.int32, (128, 256), 0) // 2 % 4
    for i in range(4):
        t1m[i] = jnp.where(rows1 == i, t1v[...].astype(F32), 0.0).astype(BF)
    for g in range(4):
        xcopies[g].wait()
        for y in range(4):
            acc = None
            for i in range(4):
                rhs = jnp.concatenate([xg[g][i, y], xg[g][i + 4, y]], axis=1)
                p = dot(t1m[i], rhs)
                acc = p if acc is None else acc + p
            acc = acc.reshape(KZ, 8, 256)
            s1[g, :, y] = jnp.concatenate([acc[:, :, :128], acc[:, :, 128:]], axis=1).astype(BF)
        if g == 0:
            pl.semaphore_wait(barrier, len(aa_peers) + len(ba_peers))
        send_aa(s1.at[g], r1.at[g], sa, ra.at[g])
        r1[g, ia] = s1[g, ia]

    for c in tcopies[2:] + wcopies:
        c.start()
    tcopies[1].wait()
    rows2 = lax.broadcasted_iota(jnp.int32, (128, 256), 0) // 2 % 2
    for i in range(2):
        t2m[i] = jnp.where(rows2 == i, t2v[...].astype(F32), 0.0).astype(BF)
    for c in tcopies[2:]:
        c.wait()
    lanes6 = lax.broadcasted_iota(jnp.int32, (256, 256), 1) // 2 % 8
    for i in range(8):
        t6m[i] = jnp.where(lanes6 == i, t6v[...].astype(F32), 0.0).astype(BF)
    half_w = (lw[...].astype(F32) * 0.5).astype(BF)
    zero_w = jnp.zeros_like(half_w)
    wbd[...] = jnp.concatenate([jnp.concatenate([half_w, zero_w], axis=1), jnp.concatenate([zero_w, half_w], axis=1)], axis=0)

    for g in range(4):
        wait_bytes(r1.at[g, pl.ds(0, NA - 1)], ra.at[g])
        acc = None
        for i in range(2):
            rhs = jnp.concatenate([r1[g, :, i].reshape(256, C), r1[g, :, i + 2].reshape(256, C)], axis=1)
            p = dot(t2m[i], rhs)
            acc = p if acc is None else acc + p
        acc = acc.reshape(KX // 2, 8, 256)
        s2[g] = jnp.concatenate([acc[:, :, :C], acc[:, :, C:]], axis=1).astype(BF)
        send_ba(lambda t: s2.at[g, pl.ds(2 * t, 2)], r2.at[g], sb, rb.at[g])
        r2[g, ib] = s2[g, pl.ds(2 * ib, 2)]

    for c in wcopies:
        c.wait()
    for g in range(3):
        wait_bytes(r2.at[g, pl.ds(0, NB - 1)], rb.at[g])
    partial = [dot(t3v[:, :384], r2[:3, :, p].reshape(384, C)) for p in range(2)]
    wait_bytes(r2.at[3, pl.ds(0, NB - 1)], rb.at[3])

    block = lax.broadcasted_iota(jnp.int32, (16, 256), 0) // 2 % 4
    row = lax.broadcasted_iota(jnp.int32, (16, C), 0)
    mixed = []
    for p in range(2):
        spec = partial[p] + dot(t3v[:, 384:], r2[3, :, p].reshape(128, C))
        keep = jnp.where(row < 8, keep_ref[0, 2 * p], keep_ref[0, 2 * p + 1])
        for q in range(8):
            lhs = jnp.concatenate([spec[16 * q:16 * q + 16], spec[128 + 16 * q:128 + 16 * q + 16]], axis=1)
            acc = None
            for j in range(4):
                k = 4 * q + j
                w = jnp.concatenate([jnp.concatenate([wv[r, 2 * p, k], wv[r, 2 * p + 1, k]], axis=1) for r in range(2)], axis=0)
                part = dot(jnp.where(block == j, lhs, 0.0).astype(BF), w)
                acc = part if acc is None else acc + part
            position = 4 * q + row // 2 % 4
            level = jnp.where(position < KY // 2, position, KY - 1 - position)
            mixed.append(jnp.where(level < keep, jnp.where(row < 8, acc[:, :C], acc[:, C:]), 0.0))
    rhs = jnp.concatenate(mixed, axis=0).astype(BF)
    for n in range(4):
        part = dot(t4v[pl.ds(256 * n, 256)], rhs).astype(BF).reshape(2, NB, 16, C)
        for h in (2 * n, 2 * n + 1):
            s3[h] = part[h - 2 * n]
            send_ba(lambda t: s3.at[h, t], r3.at[h], sc, rc.at[h])
            r3[h, ib] = s3[h, ib]

    for g in range(4):
        for n in range(2):
            wait_bytes(r3.at[2 * g + n, pl.ds(0, NB - 1)], rc.at[2 * g + n])
            rhs = r3[2 * g + n].reshape(128, C)
            for i in range(2):
                s4[g, :, 2 * n + i] = dot(t5v[pl.ds(256 * i, 256)], rhs).astype(BF).reshape(NA, 16, C)
            if g == 0:
                for t in aa_peers:
                    pltpu.make_async_remote_copy(s4.at[g, t, pl.ds(2 * n, 2)], r4.at[g, ia, pl.ds(2 * n, 2)], sd, rd.at[g], device_id={"aa": t}, device_id_type=MESH).start()
        land = r4.at[g] if g < 3 else blast
        if g == 3:
            for t in EARLY_FIRST:
                @pl.when(ia != t)
                def _():
                    pltpu.make_async_remote_copy(s4.at[g, t], land.at[ia], sd, rd.at[g], device_id={"aa": t}, device_id_type=MESH).start()
        elif g > 0:
            send_aa(s4.at[g], land, sd, rd.at[g])
        land[ia] = s4[g, ia]

    bias = bias_row(bias_ref)
    for g in range(3):
        wait_bytes(r4.at[g, pl.ds(0, NA - 1)], rd.at[g])
        for y in (0, 2):
            rhs = back_pair(r4.at[g], y)
            for x in range(8):
                o = combine(xv[g, x, y], xv[g, x, y + 1], wbd[...], t6m[x], rhs, bias)
                out_ref[x, 4 * g + y] = o[:, :C]
                out_ref[x, 4 * g + y + 1] = o[:, C:]

    wait_bytes(blast.at[pl.ds(0, NA - 1)], rd.at[3])
    wait_bytes(s1.at[:, pl.ds(0, NA - 1)], sa)
    wait_bytes(s4.at[:, pl.ds(0, NA - 1)], sd)
    wait_bytes(r2.at[:, pl.ds(0, NB - 1)], sb)
    wait_bytes(r3.at[:, pl.ds(0, NB - 1)], sc)


def store_kernel(val_ref, xlast, blast, t6m, wbd, bias_ref, out_ref, tail, sem):
    copies = [pltpu.make_async_copy(val_ref.at[i], out_ref.at[i, pl.ds(0, 12)], sem.at[i]) for i in range(8)]
    tails = [pltpu.make_async_copy(tail.at[i], out_ref.at[i, pl.ds(12, 4)], sem.at[8 + i]) for i in range(8)]
    for c in copies:
        c.start()
    bias = bias_row(bias_ref)
    rhs = [back_pair(blast, y) for y in (0, 2)]
    for x in range(8):
        for i in range(2):
            o = combine(xlast[x, 2 * i], xlast[x, 2 * i + 1], wbd[...], t6m[x], rhs[i], bias)
            tail[x, 2 * i] = o[:, :C]
            tail[x, 2 * i + 1] = o[:, C:]
        if x > 0:
            tails[x - 1].start()
    tails[7].start()
    for c in copies + tails:
        c.wait()


def per_device(grid_features, weight_real, weight_imag, mode_keep, local_weight, local_bias):
    t1, t2, t3, t4, t5, t6 = tables()
    any_spec = pl.BlockSpec(memory_space=pltpu.HBM)
    vmem_spec = pl.BlockSpec(memory_space=pltpu.VMEM)
    V = lambda *s: pltpu.VMEM(s, BF)
    D = pltpu.SemaphoreType.DMA
    hbm = lambda a: pltpu.with_memory_space_constraint(a, pltpu.HBM)
    results = pl.pallas_call(
        spectral_kernel,
        out_shape=[jax.ShapeDtypeStruct(shape, BF) for shape in (
            (8, 12, NZ, C), (8, 4, NZ, C), (NA, 4, 16, C), (8, 256, 256), (256, 256))],
        in_specs=[any_spec] * 12,
        out_specs=[vmem_spec] * 5,
        scratch_shapes=[
            V(3, 8, 4, NZ, C), V(2, 4, KY, C, C), pltpu.SMEM((1, 4), jnp.int32), V(128, 256), V(4, 128, 256),
            V(128, 256), V(2, 128, 256), V(256, 512), V(1024, 256), V(512, 128), V(256, 256), V(C, C), V(1, C),
            V(4, NA, 4, 16, C), V(4, NA, 4, 16, C), V(4, KX // 2, 16, C), V(4, NB, 2, 16, C),
            V(8, NB, 16, C), V(8, NB, 16, C), V(4, NA, 4, 16, C), V(3, NA, 4, 16, C),
            D((4,)), D((3,)), D((8,)), D(()), D((4,)), D(()), D((4,)), D(()), D((8,)), D(()), D((4,)),
        ],
        compiler_params=pltpu.CompilerParams(collective_id=0, has_side_effects=True, vmem_limit_bytes=40 << 20),
        name="spectral",
    )(*map(hbm, (grid_features, weight_real.reshape(4, KY, C, C), weight_imag.reshape(4, KY, C, C), mode_keep.reshape(1, 4),
                 *map(jnp.asarray, (t1, t2, t3, t4, t5, t6)), local_weight, local_bias.reshape(1, C))))

    return pl.pallas_call(
        store_kernel,
        out_shape=jax.ShapeDtypeStruct((8, 16, NZ, C), BF),
        in_specs=[vmem_spec] * 6,
        out_specs=any_spec,
        scratch_shapes=[V(8, 4, NZ, C), D((16,))],
        compiler_params=pltpu.CompilerParams(vmem_limit_bytes=6 << 20),
        name="store",
    )(*results, local_bias.reshape(1, C))


def solution(mesh):
    in_specs = (P("aa", "ba", None, None), P("ba", None, "aa", None, None), P("ba", None, "aa", None, None),
                P("ba", "aa"), P(), P())
    return jax.shard_map(per_device, mesh=mesh, in_specs=in_specs, out_specs=P("aa", "ba", None, None), check_vma=False)
```
